32 devices in a mesh: groups: 2 (over x), dp: 4 (over y, core), fsdp: 4 (over z).
Axes of the slice: x: 2, y: 2, z: 4, core: 2. Of those that a mesh axis runs over, the one named last changes fastest.
Arguments:
- tokens: bfloat16 [4096, 4096], P(('groups', 'dp', 'fsdp')), parts along dimension 0, may hold values from -6 to 6
- up_weight: bfloat16 [4096, 14336], P('fsdp', 'dp'), may hold values from -0.09375 to 0.09375
- first_adapter_factors: bfloat16 [32, 32, 4096], P(('groups', 'dp', 'fsdp')), parts along dimension 0, may hold values from -0.09375 to 0.09375
- second_adapter_factors: bfloat16 [32, 32, 14336], P(('groups', 'dp', 'fsdp')), parts along dimension 0, may hold values from -1 to 1
- counts: int32 [32], P(('groups', 'dp', 'fsdp')), parts along dimension 0, may hold values from 1 to 128, as said below
- output_gradient: bfloat16 [4096, 14336], P(('groups', 'dp', 'fsdp')), parts along dimension 0, may hold values from -6 to 6
Outputs:
- act_out: bfloat16 [4096, 14336], P(('groups', 'dp', 'fsdp')), parts along dimension 0
- grad_a: float32 [32, 32, 4096], P(('groups', 'dp', 'fsdp')), parts along dimension 0
- second_factor_gradient: float32 [32, 32, 14336], P(('groups', 'dp', 'fsdp')), parts along dimension 0
The draws below stay inside these ranges and needn't reach their ends.
There are 2 independent parts, one for each index of `groups`. The reference program is written for one: setup_inputs(seed, part) draws one part's arguments, and reference() takes and returns one part's arrays. A program takes and returns all parts, laid end to end along the dimension named above; an argument that names none is the same for every part. Nothing has to cross between parts.
Inputs may be any that keep to these rules, and one draw needn't show every extreme that they name: counts[d] is the number of live rows of adapter d. For d < 8, counts[d] + counts[d + 8] <= 160; in every draw some such pair has the counts 128 and 32.
All inputs are finite; a program needn't handle non-finite values.
Results may differ from the reference program's by a relative error of at most 0.0058.
Values may be sent and summed in bfloat16 or wider, within the bound.
No kernel may reach another device: no remote copies, remote signals or barrier semaphores. Data moves between devices by JAX's collectives and lax.ppermute only.
A program may use at most 128 MiB of HBM per device.

```python
import jax
import jax.numpy as jnp

INPUT_WIDTH = 4096
HIDDEN_WIDTH = 14336
ADAPTER_RANK = 32
SLOTS = 128
PAIR_ROWS = 80
TENANT_ADAPTERS = 16
ROWS = 2048
N_DP = 4
N_FSDP = 4


def draw_counts(key, part):
    half_dp = N_DP // 2
    pair_total = half_dp * N_FSDP
    first_key, second_key, flip_key, forced_key = jax.random.split(jax.random.fold_in(key, 17), 4)
    first_count = jax.random.randint(first_key, (pair_total,), 1, SLOTS + 1)
    forced = jax.random.randint(forced_key, (), 0, pair_total)
    marker = jnp.arange(pair_total) == forced
    first_count = jnp.where(marker, SLOTS, first_count)
    count_limit = jnp.minimum(SLOTS, 2 * PAIR_ROWS - first_count)
    second_count = jax.random.randint(second_key, (pair_total,), 1, count_limit + 1)
    second_count = jnp.where(marker, 2 * PAIR_ROWS - SLOTS, second_count)
    flipped = jax.random.randint(flip_key, (pair_total,), 0, 2) == 1
    low_half = jnp.where(flipped, second_count, first_count).reshape(half_dp, N_FSDP)
    high_half = jnp.where(flipped, first_count, second_count).reshape(half_dp, N_FSDP)
    return jnp.concatenate([low_half, high_half], 0).reshape(N_DP * N_FSDP).astype(jnp.int32)


def levels(rng, extent, shards, smallest, largest):
    loudness, own = 1.0, jax.random.fold_in(rng, 6)
    for axis_at, shards_of in shards:
        heights = jnp.exp(jax.random.uniform(jax.random.fold_in(own, axis_at), (shards_of,), jnp.float32, smallest / len(shards), largest / len(shards)))
        loudness = loudness * jnp.repeat(heights, extent[axis_at] // shards_of).reshape([-1 if axis == axis_at else 1 for axis in range(len(extent))])
    return loudness


def normal_values(key, dims, scale, limit, cuts=(), kind=jnp.bfloat16):
    gain = levels(key, dims, cuts, -0.22, 0.18) if cuts else 1.0
    entries = jax.random.normal(key, dims, jnp.float32) * scale * gain
    return jnp.minimum(jnp.maximum(entries, -limit), limit).astype(kind)


def setup_inputs(seed: int = 0, part: int = 0) -> dict:
    keys = jax.random.split(jax.random.key(seed), 7)
    part_splits = jax.random.split(jax.random.fold_in(keys[6], part), 7)
    tokens = normal_values(part_splits[0], (ROWS, INPUT_WIDTH), 1.0, 6.0, ((0, 16),))
    up_weight = normal_values(keys[1], (INPUT_WIDTH, HIDDEN_WIDTH), INPUT_WIDTH ** -0.5, 0.09375, ((0, 4), (1, 4)))
    first_adapter_factors = normal_values(part_splits[2], (TENANT_ADAPTERS, ADAPTER_RANK, INPUT_WIDTH), INPUT_WIDTH ** -0.5, 0.09375, ((0, 16),))
    second_adapter_factors = normal_values(part_splits[3], (TENANT_ADAPTERS, ADAPTER_RANK, HIDDEN_WIDTH), ADAPTER_RANK ** -0.5, 1.0, ((0, 16),))
    counts = draw_counts(jax.random.fold_in(jax.random.fold_in(keys[6], part), 71), part)
    output_gradient = normal_values(part_splits[5], (ROWS, HIDDEN_WIDTH), 1.0, 6.0, ((0, 16),))
    return {"tokens": tokens, "up_weight": up_weight, "first_adapter_factors": first_adapter_factors, "second_adapter_factors": second_adapter_factors, "counts": counts, "output_gradient": output_gradient}


LOWRANK_SCALE = 2.0


def silu_slope(inputs):
    gate_value = jax.nn.sigmoid(inputs)
    return gate_value * (1.0 + inputs * (1.0 - gate_value))


def reference(tokens, up_weight, first_adapter_factors, second_adapter_factors, counts, output_gradient):
    positions = jnp.arange(SLOTS, dtype=jnp.int32)
    live_rows = (positions[None, :] < counts[:, None]).reshape(TENANT_ADAPTERS * SLOTS, 1)
    base_output = jnp.dot(tokens, up_weight, preferred_element_type=jnp.float32).astype(jnp.bfloat16)
    grouped = tokens.reshape(TENANT_ADAPTERS, SLOTS, INPUT_WIDTH).astype(jnp.float32)
    down_factor = first_adapter_factors.astype(jnp.float32)
    up_factor = second_adapter_factors.astype(jnp.float32)
    rank_projection = jnp.einsum("asd,ard->asr", grouped, down_factor).astype(jnp.bfloat16)
    adapter_update = jnp.einsum("asr,arf->asf", rank_projection.astype(jnp.float32), up_factor).reshape(TENANT_ADAPTERS * SLOTS, HIDDEN_WIDTH)
    hidden_preactivation = base_output.astype(jnp.float32) + LOWRANK_SCALE * adapter_update
    act_out = jnp.where(live_rows, jax.nn.silu(hidden_preactivation), 0.0).astype(jnp.bfloat16)
    grad_pre = jnp.where(live_rows, output_gradient.astype(jnp.float32) * silu_slope(hidden_preactivation), 0.0).astype(jnp.bfloat16)
    grouped_gradient = grad_pre.reshape(TENANT_ADAPTERS, SLOTS, HIDDEN_WIDTH).astype(jnp.float32)
    low_rank_gradient = (LOWRANK_SCALE * jnp.einsum("vcn,vdn->vcd", grouped_gradient, up_factor)).astype(jnp.bfloat16)
    second_factor_gradient = LOWRANK_SCALE * jnp.einsum("tbi,tbd->tid", rank_projection.astype(jnp.float32), grouped_gradient)
    grad_a = jnp.einsum("asr,asd->ard", low_rank_gradient.astype(jnp.float32), grouped)
    return act_out, grad_a, second_factor_gradient
```

```python
import jax
import jax.numpy as jnp
from jax import lax
from jax.sharding import PartitionSpec as P

SLOTS = 128
PAIR_ROWS = 80


LOWRANK_SCALE = 2.0


def partner(x, axis, distance):
    return lax.ppermute(x, axis, [(i, i ^ 1 << distance) for i in range(lax.axis_size(axis))])


def silu_slope(inputs):
    gate_value = jax.nn.sigmoid(inputs)
    return gate_value * (1.0 + inputs * (1.0 - gate_value))


def take_block(rows_all, offset, row_count):
    filler = jnp.zeros((row_count,) + rows_all.shape[1:], rows_all.dtype)
    padded = jnp.concatenate([rows_all, filler], 0)
    return lax.dynamic_slice_in_dim(padded, offset, row_count, 0)


def place_block(rows_kept, block, offset, row_total):
    filler = jnp.zeros((block.shape[0],) + rows_kept.shape[1:], rows_kept.dtype)
    padded = jnp.concatenate([rows_kept, filler], 0)
    placed = lax.dynamic_update_slice_in_dim(padded, block, offset, 0)
    return placed[:row_total]


def per_device(
    tokens, up_weight, first_adapter_factors, second_adapter_factors, counts, output_gradient
):
    down_factor = first_adapter_factors[0]
    up_factor = second_adapter_factors[0]
    slot_total = tokens.shape[0]
    own_count = counts[0]
    live_rows = jnp.arange(slot_total, dtype=jnp.int32)[:, None] < own_count
    spare_rows = SLOTS - PAIR_ROWS
    half_bit = lax.axis_size("dp").bit_length() - 2
    kept_rows = jnp.minimum(own_count, PAIR_ROWS)
    outgoing = take_block(tokens, kept_rows, spare_rows)
    guest = partner(outgoing, "dp", half_bit)
    paired_rows = place_block(tokens[:PAIR_ROWS], guest, kept_rows, PAIR_ROWS)
    dp_total, fsdp_total = lax.axis_size("dp"), lax.axis_size("fsdp")
    sliced_rows = lax.all_to_all(paired_rows, "fsdp", split_axis=1, concat_axis=0, tiled=True)
    slice_width = sliced_rows.shape[1]
    all_rows = lax.all_gather(sliced_rows, "dp", axis=0, tiled=True)
    all_rows = all_rows.reshape(dp_total, fsdp_total, PAIR_ROWS, slice_width).swapaxes(0, 1)
    partial_blocks = jnp.dot(
        all_rows.reshape(-1, slice_width), up_weight, preferred_element_type=jnp.float32
    ).astype(jnp.bfloat16)
    blocks = lax.psum_scatter(partial_blocks, "fsdp", scatter_dimension=0, tiled=True)
    paired_base = lax.all_to_all(blocks, "dp", split_axis=0, concat_axis=1, tiled=True)
    returned = partner(take_block(paired_base, kept_rows, spare_rows), "dp", half_bit)
    base_output = place_block(paired_base, returned, kept_rows, SLOTS)
    rank_projection = lax.dot_general(
        tokens, down_factor, (((1,), (1,)), ((), ())), preferred_element_type=jnp.float32
    ).astype(jnp.bfloat16)
    adapter_update = jnp.dot(rank_projection, up_factor, preferred_element_type=jnp.float32)
    hidden_preactivation = base_output.astype(jnp.float32) + LOWRANK_SCALE * adapter_update
    act_out = jnp.where(live_rows, jax.nn.silu(hidden_preactivation), 0.0).astype(jnp.bfloat16)
    grad_pre = jnp.where(
        live_rows, output_gradient.astype(jnp.float32) * silu_slope(hidden_preactivation), 0.0
    ).astype(jnp.bfloat16)
    low_rank_gradient = (
        LOWRANK_SCALE
        * lax.dot_general(
            grad_pre, up_factor, (((1,), (1,)), ((), ())), preferred_element_type=jnp.float32
        )
    ).astype(jnp.bfloat16)
    second_factor_gradient = LOWRANK_SCALE * lax.dot_general(
        rank_projection, grad_pre, (((0,), (0,)), ((), ())), preferred_element_type=jnp.float32
    )
    grad_a = lax.dot_general(
        low_rank_gradient, tokens, (((0,), (0,)), ((), ())), preferred_element_type=jnp.float32
    )
    return (act_out, grad_a[None], second_factor_gradient[None])


def solution(mesh):
    placed = (
        P(("groups", "dp", "fsdp"), None),
        P("fsdp", "dp"),
        P(("groups", "dp", "fsdp"), None, None),
        P(("groups", "dp", "fsdp"), None, None),
        P(("groups", "dp", "fsdp")),
        P(("groups", "dp", "fsdp"), None),
    )
    return jax.shard_map(
        per_device,
        mesh=mesh,
        in_specs=placed,
        out_specs=(
            P(("groups", "dp", "fsdp"), None),
            P(("groups", "dp", "fsdp"), None, None),
            P(("groups", "dp", "fsdp"), None, None),
        ),
        check_vma=False,
    )
```

```python
import functools

import jax
import jax.numpy as jnp
from jax import lax
from jax.experimental import pallas as pl
from jax.experimental.pallas import tpu as pltpu
from jax.sharding import PartitionSpec as P


SLOTS = 128
PAIR_ROWS = 80


LOWRANK_SCALE = 2.0


def partner(x, axis, distance):
    return lax.ppermute(x, axis, [(i, i ^ 1 << distance) for i in range(lax.axis_size(axis))])


def silu_slope(inputs):
    gate_value = jax.nn.sigmoid(inputs)
    return gate_value * (1.0 + inputs * (1.0 - gate_value))


def take_block(rows_all, offset, row_count):
    filler = jnp.zeros((row_count,) + rows_all.shape[1:], rows_all.dtype)
    padded = jnp.concatenate([rows_all, filler], 0)
    return lax.dynamic_slice_in_dim(padded, offset, row_count, 0)


def place_block(rows_kept, block, offset, row_total):
    filler = jnp.zeros((block.shape[0],) + rows_kept.shape[1:], rows_kept.dtype)
    padded = jnp.concatenate([rows_kept, filler], 0)
    placed = lax.dynamic_update_slice_in_dim(padded, block, offset, 0)
    return placed[:row_total]


def after(x, *others):
    return lax.optimization_barrier((x,) + others)[0]


def scattered_plan(
    tokens, up_weight, down_factor, up_factor, own_count, output_gradient
):
    dp_total, fsdp_total = lax.axis_size("dp"), lax.axis_size("fsdp")
    live_rows = jnp.arange(tokens.shape[0], dtype=jnp.int32)[:, None] < own_count
    spare_rows = SLOTS - PAIR_ROWS
    half_bit = dp_total.bit_length() - 2
    kept_rows = jnp.minimum(own_count, PAIR_ROWS)
    guest = partner(take_block(tokens, kept_rows, spare_rows), "dp", half_bit)
    packed = place_block(tokens[:PAIR_ROWS], guest, kept_rows, PAIR_ROWS)
    sliced_rows = lax.all_to_all(packed, "fsdp", split_axis=1, concat_axis=0, tiled=True)
    slice_width = sliced_rows.shape[1]
    all_rows = lax.all_gather(sliced_rows, "dp", axis=0, tiled=True)
    all_rows = all_rows.reshape(dp_total, fsdp_total, PAIR_ROWS, slice_width).swapaxes(0, 1)
    partial_blocks = jnp.dot(
        all_rows.reshape(-1, slice_width), up_weight, preferred_element_type=jnp.float32
    ).astype(jnp.bfloat16)
    blocks = lax.psum_scatter(partial_blocks, "fsdp", scatter_dimension=0, tiled=True)
    paired_base = lax.all_to_all(blocks, "dp", split_axis=0, concat_axis=1, tiled=True)
    returned = partner(take_block(paired_base, kept_rows, spare_rows), "dp", half_bit)
    base_output = place_block(paired_base, returned, kept_rows, SLOTS)
    rank_projection = lax.dot_general(
        tokens, down_factor, (((1,), (1,)), ((), ())), preferred_element_type=jnp.float32
    ).astype(jnp.bfloat16)
    adapter_update = jnp.dot(rank_projection, up_factor, preferred_element_type=jnp.float32)
    hidden_preactivation = base_output.astype(jnp.float32) + LOWRANK_SCALE * adapter_update
    act_out = jnp.where(live_rows, jax.nn.silu(hidden_preactivation), 0.0).astype(jnp.bfloat16)
    grad_pre = jnp.where(
        live_rows, output_gradient.astype(jnp.float32) * silu_slope(hidden_preactivation), 0.0
    ).astype(jnp.bfloat16)
    low_sum = lax.dot_general(
        grad_pre, up_factor, (((1,), (1,)), ((), ())), preferred_element_type=jnp.float32
    )
    second_factor_gradient = LOWRANK_SCALE * lax.dot_general(
        rank_projection, grad_pre, (((0,), (0,)), ((), ())), preferred_element_type=jnp.float32
    )
    return act_out, low_sum, second_factor_gradient


def tail_kernel(
    slots_ref, counts_ref, own_ref, beside_ref, across_ref, diagonal_ref, rank_ref, rank_t_ref,
    turn_ref, factor_ref, cotangent_ref, low_in_ref, *rest
):
    act_ref, second_ref, low_ref, base_ref = rest[-4:]
    which, tile = pl.program_id(0), pl.program_id(1)

    @pl.when((which == 0) & (tile == 0))
    def _():
        low_ref[...] = low_in_ref[...]

    for index, source_ref in enumerate((own_ref, beside_ref, across_ref, diagonal_ref)):

        @pl.when(which == index)
        def _(source_ref=source_ref):
            base_ref[...] = source_ref[...]

    base = jnp.dot(turn_ref[...], base_ref[...], preferred_element_type=jnp.float32)
    factor = factor_ref[...]
    update = jnp.dot(rank_ref[...], factor, preferred_element_type=jnp.float32)
    inputs = base + LOWRANK_SCALE * update
    gate_value = jax.nn.sigmoid(inputs)
    live = lax.broadcasted_iota(jnp.int32, inputs.shape, 0) < counts_ref[0]
    act_ref[...] = jnp.where(live, inputs * gate_value, 0.0).astype(jnp.bfloat16)
    slope = gate_value * (1.0 + inputs * (1.0 - gate_value))
    grad_pre = cotangent_ref[...].astype(jnp.float32) * slope
    grad_pre = jnp.where(live, grad_pre, 0.0).astype(jnp.bfloat16)
    second_ref[...] = LOWRANK_SCALE * jnp.dot(
        rank_t_ref[...], grad_pre, preferred_element_type=jnp.float32
    )
    low_ref[...] += lax.dot_general(
        grad_pre, factor, (((1,), (1,)), ((), ())), preferred_element_type=jnp.float32
    )


def tail(bases, rank, rank_t, turn, factor, cotangent, low, made, slots, count, offset, unit):
    width = bases[0].shape[1]
    rank_total, hidden = factor.shape
    start = offset // unit

    def local(i, t, slots, counts):
        return (0, t)

    def whole(i, t, slots, counts):
        return (0, 0)

    def placed(i, t, slots, counts):
        return (0, slots[i] + start + t)

    in_specs = [pl.BlockSpec((SLOTS, unit), local)] * 4 + [
        pl.BlockSpec(rank.shape, whole),
        pl.BlockSpec(rank_t.shape, whole),
        pl.BlockSpec(turn.shape, whole),
        pl.BlockSpec((rank_total, unit), placed),
        pl.BlockSpec((SLOTS, unit), placed),
        pl.BlockSpec(low.shape, whole),
    ]
    operands = [*bases, rank, rank_t, turn, factor, cotangent, low]
    aliases = {}
    if made is not None:
        in_specs += [pl.BlockSpec(memory_space=pl.ANY)] * 2
        aliases = {2 + len(operands): 0, 3 + len(operands): 1}
        operands += list(made)
    act_out, second, low = pl.pallas_call(
        tail_kernel,
        name="tail",
        out_shape=(
            jax.ShapeDtypeStruct((SLOTS, hidden), jnp.bfloat16),
            jax.ShapeDtypeStruct((rank_total, hidden), jnp.float32),
            jax.ShapeDtypeStruct(low.shape, jnp.float32),
        ),
        grid_spec=pltpu.PrefetchScalarGridSpec(
            num_scalar_prefetch=2,
            grid=(4, width // unit),
            in_specs=in_specs,
            out_specs=(
                pl.BlockSpec((SLOTS, unit), placed),
                pl.BlockSpec((rank_total, unit), placed),
                pl.BlockSpec(low.shape, whole),
            ),
            scratch_shapes=[pltpu.VMEM((SLOTS, unit), jnp.bfloat16)],
        ),
        input_output_aliases=aliases,
        cost_estimate=pl.CostEstimate(
            flops=2 * 4 * width * SLOTS * (SLOTS + 3 * rank_total),
            bytes_accessed=4 * width * SLOTS * 8,
            transcendentals=4 * width * SLOTS,
        ),
        compiler_params=pltpu.CompilerParams(
            dimension_semantics=("arbitrary", "arbitrary"), vmem_limit_bytes=6 * 2**20
        ),
    )(slots, count, *operands)
    return (act_out, second), low


def chunk_plan(width):
    if width % (7 * 128) == 0:
        return width // 7, (1,) * 7, (2, 2, 2, 1)
    for total in (8, 4, 2):
        if width % (total * 128) == 0:
            return width // total, (1,) * total, (1,) * total
    return width, (1,), (1,)


def plane_plan(
    tokens, up_weight, down_factor, up_factor, own_count, output_gradient
):
    groups = lax.axis_size("groups")
    place, group = lax.axis_index("fsdp"), lax.axis_index("groups")
    position = lax.axis_index("dp")
    upper = position >= 2
    inner = (place == 1) | (place == 2)
    near = jnp.where(place < 2, 1, 2)
    far = 3 - near
    slice_width, width = up_weight.shape
    part = slice_width // groups
    unit, sizes, batches = chunk_plan(width)
    chunks = len(sizes)
    offsets = [sum(sizes[:c]) * unit for c in range(chunks)]
    spare = SLOTS - PAIR_ROWS
    pair_total = 2 * PAIR_ROWS
    home_total = 2 * pair_total
    beside = [(0, 1), (1, 0), (2, 3), (3, 2)]
    across = [(0, 2), (2, 0), (1, 3), (3, 1)]
    diagonal = [(0, 3), (3, 0), (1, 2), (2, 1)]
    inward = [(0, 1), (3, 2)]
    outward = [(1, 0), (2, 3)]
    middle = [(1, 2), (2, 1)]
    crossing = [(0, 2), (3, 1)]

    row = jnp.arange(SLOTS, dtype=jnp.int32)
    source = jnp.where(upper, SLOTS - 1 - row, row)
    turn = (source[:, None] == row[None, :]).astype(jnp.bfloat16)
    ordered = jnp.dot(turn, tokens, preferred_element_type=jnp.float32).astype(jnp.bfloat16)
    spill = jnp.where(upper, ordered[:spare], ordered[PAIR_ROWS:])
    guest = lax.ppermute(spill, "dp", across)

    def own_part(weight, c):
        return lax.dynamic_slice(
            weight, (group * part, offsets[c]), (part, sizes[c] * unit)
        )

    first_part = own_part(after(up_weight, spill), 0)
    lines = {0: lax.ppermute(first_part, "fsdp", inward)}
    rest_weight = after(up_weight, first_part)
    parts = [first_part] + [own_part(rest_weight, c) for c in range(1, chunks)]
    column_weights = [
        rest_weight[:, offsets[c] : offsets[c] + sizes[c] * unit] for c in range(chunks)
    ]
    guest, *column_weights = lax.optimization_barrier((guest, *column_weights))

    spot = jnp.where(upper, PAIR_ROWS, 0) + jnp.arange(PAIR_ROWS, dtype=jnp.int32)[:, None]
    is_own = jnp.where(upper, pair_total - 1 - spot, spot) < own_count
    kept = jnp.where(upper, ordered[spare:], ordered[:PAIR_ROWS])
    blank = jnp.zeros((PAIR_ROWS - spare, guest.shape[1]), guest.dtype)
    placed = jnp.where(
        upper, jnp.concatenate([guest, blank], 0), jnp.concatenate([blank, guest], 0)
    )
    touched = (spot >= PAIR_ROWS - spare) & (spot < SLOTS)
    packed = jnp.where(touched & ~is_own, placed, kept)

    def columns(target):
        outer = jnp.where(target < 2, 0, 3)
        pieces = [lax.dynamic_slice_in_dim(packed, target * slice_width, slice_width, 1)]
        for step in range(groups):
            origin = outer * slice_width + lax.rem(group + step, groups) * part
            pieces.append(lax.dynamic_slice_in_dim(packed, origin, part, 1))
        return jnp.concatenate(pieces, 1)

    def start_weight(c, *order):
        return lax.ppermute(after(parts[c], *order), "fsdp", inward)

    def share_weight(c, *order):
        line = lines[c]
        pieces = [line]
        line = after(line, *order)
        for step in range(1, groups):
            pairs = [(i, (i - step) % groups) for i in range(groups)]
            pieces.append(lax.ppermute(line, "groups", pairs))
        return pieces

    def ordered_pair(mine):
        theirs = lax.ppermute(mine, "dp", across)
        return jnp.concatenate(
            [jnp.where(upper, theirs, mine), jnp.where(upper, mine, theirs)], 0
        )

    far_columns = columns(far)
    from_far = lax.ppermute(far_columns, "fsdp", middle)
    near_columns = columns(near)
    from_outer = lax.ppermute(near_columns, "fsdp", inward)
    from_far_outer = lax.ppermute(far_columns, "fsdp", crossing)
    shared = {0: share_weight(0, near_columns)}
    near_pair = ordered_pair(near_columns)
    for c in range(1, min(3, chunks)):
        lines[c] = start_weight(c, near_columns)
    far_pair = ordered_pair(from_far)
    far_outer_pair = ordered_pair(from_far_outer)
    far_pairs = jnp.concatenate([far_pair, far_outer_pair], 0)
    far_others = lax.ppermute(far_pairs, "dp", beside)
    if chunks > 1:
        shared[1] = share_weight(1, far_pairs)
    far_rows = jnp.concatenate(
        [far_pair, far_others[:pair_total], far_outer_pair, far_others[pair_total:]], 0
    )
    outer_pair = ordered_pair(after(from_outer, far_pairs))
    near_pairs = jnp.concatenate([near_pair, outer_pair], 0)
    near_others = lax.ppermute(after(near_pairs, far_rows), "dp", beside)

    rank = lax.dot_general(
        tokens, down_factor, (((1,), (1,)), ((), ())), preferred_element_type=jnp.float32
    ).astype(jnp.bfloat16)
    rank_t = rank.T
    slots = (position ^ jnp.arange(4, dtype=jnp.int32)) * (width // unit)
    low = jnp.zeros((SLOTS, rank.shape[1]), jnp.float32)
    count = own_count.reshape(1)

    def send(c, *order):
        weight = jnp.concatenate([column_weights[c]] + shared[c], 0)
        rows = after(far_rows, *order) if order else far_rows
        outgoing = jnp.dot(rows, weight, preferred_element_type=jnp.float32)
        outgoing = outgoing.astype(jnp.bfloat16)
        return weight, outgoing, lax.ppermute(outgoing, "fsdp", middle)

    sent = {0: send(0)}
    last = sent[0][1]
    near_others = after(near_others, last)
    near_rows = jnp.concatenate(
        [near_pair, near_others[:pair_total], outer_pair, near_others[pair_total:]], 0
    )

    def finish(c, *order):
        weight, _, incoming = sent[c]
        rows = after(near_rows, *order)
        summed = jnp.dot(rows, weight, preferred_element_type=jnp.float32)
        summed = (summed + incoming.astype(jnp.float32)).astype(jnp.bfloat16)
        return summed, lax.ppermute(summed[home_total:], "fsdp", outward)

    def hand_out(members, *order):
        handed = [after(handed, *order) for _, handed in members]
        homes = [
            jnp.where(inner, summed[:home_total], back)
            for (summed, _), back in zip(members, handed, strict=True)
        ]
        home = jnp.concatenate(homes, 1).reshape(2, pair_total, -1)
        shape = (1, SLOTS, home.shape[2])
        same, other = jnp.where(upper, pair_total - SLOTS, 0), jnp.where(upper, 0, pair_total - SLOTS)
        cuts = [
            lax.dynamic_slice(home, (pair, row_at, 0), shape)[0]
            for pair, row_at in ((0, same), (1, same), (0, other), (1, other))
        ]
        opposite = lax.ppermute(cuts[2], "dp", across)
        cornered = lax.ppermute(cuts[3], "dp", diagonal)
        adjacent = lax.ppermute(cuts[1], "dp", beside)
        return cuts, [cuts[0], adjacent, opposite, cornered]

    batch_ends = [sum(batches[: b + 1]) - 1 for b in range(len(batches))]
    made = None
    summed, pending = {}, []
    for i in range(chunks + 1):
        if i + 3 < chunks:
            lines[i + 3] = start_weight(i + 3, last)
        if i + 2 < chunks:
            shared[i + 2] = share_weight(i + 2, last)
        if i + 1 < chunks:
            sent[i + 1] = send(i + 1, last)
            last = sent[i + 1][1]
        if i < chunks:
            summed[i] = finish(i, last)
            last = summed[i][0]
        if pending and (i < chunks or len(pending) > 1):
            bases, offset = pending.pop(0)
            bases[3] = after(bases[3], last)
            made, low = tail(
                bases, rank, rank_t, turn, up_factor, output_gradient, low, made, slots, count,
                offset, unit,
            )
            last = low
        if i - 1 in batch_ends:
            b = batch_ends.index(i - 1)
            begin = batch_ends[b] - batches[b] + 1
            cuts, bases = hand_out([summed[c] for c in range(begin, i)], last)
            pending.append((bases, offsets[begin]))
            last = cuts[0]
    for bases, offset in pending:
        bases[3] = after(bases[3], last)
        made, low = tail(
            bases, rank, rank_t, turn, up_factor, output_gradient, low, made, slots, count,
            offset, unit,
        )
        last = low
    return made[0], low, made[1]


def per_device(
    plan, tokens, up_weight, first_adapter_factors, second_adapter_factors, counts, output_gradient
):
    act_out, low_sum, second_factor_gradient = plan(
        tokens, up_weight, first_adapter_factors[0], second_adapter_factors[0], counts[0],
        output_gradient,
    )
    low_rank_gradient = (LOWRANK_SCALE * low_sum).astype(jnp.bfloat16)
    grad_a = lax.dot_general(
        low_rank_gradient, tokens, (((0,), (0,)), ((), ())), preferred_element_type=jnp.float32
    )
    return (act_out, grad_a[None], second_factor_gradient[None])


def solution(mesh):
    placed = (
        P(("groups", "dp", "fsdp"), None),
        P("fsdp", "dp"),
        P(("groups", "dp", "fsdp"), None, None),
        P(("groups", "dp", "fsdp"), None, None),
        P(("groups", "dp", "fsdp")),
        P(("groups", "dp", "fsdp"), None),
    )

    def mapped(plan):
        return jax.shard_map(
            functools.partial(per_device, plan),
            mesh=mesh,
            in_specs=placed,
            out_specs=(
                P(("groups", "dp", "fsdp"), None),
                P(("groups", "dp", "fsdp"), None, None),
                P(("groups", "dp", "fsdp"), None, None),
            ),
            check_vma=False,
        )

    if mesh.shape["fsdp"] == 4 and mesh.shape["dp"] == 4:
        return mapped(plane_plan)
    return mapped(scattered_plan)
```

```python
import functools

import jax
import jax.numpy as jnp
from jax import lax
from jax.experimental import pallas as pl
from jax.experimental.pallas import tpu as pltpu
from jax.sharding import PartitionSpec as P


SLOTS = 128
PAIR_ROWS = 80


LOWRANK_SCALE = 2.0


def partner(x, axis, distance):
    return lax.ppermute(x, axis, [(i, i ^ 1 << distance) for i in range(lax.axis_size(axis))])


def silu_slope(inputs):
    gate_value = jax.nn.sigmoid(inputs)
    return gate_value * (1.0 + inputs * (1.0 - gate_value))


def take_block(rows_all, offset, row_count):
    filler = jnp.zeros((row_count,) + rows_all.shape[1:], rows_all.dtype)
    padded = jnp.concatenate([rows_all, filler], 0)
    return lax.dynamic_slice_in_dim(padded, offset, row_count, 0)


def place_block(rows_kept, block, offset, row_total):
    filler = jnp.zeros((block.shape[0],) + rows_kept.shape[1:], rows_kept.dtype)
    padded = jnp.concatenate([rows_kept, filler], 0)
    placed = lax.dynamic_update_slice_in_dim(padded, block, offset, 0)
    return placed[:row_total]


def after(x, *others):
    return lax.optimization_barrier((x,) + others)[0]


def scattered_plan(
    tokens, up_weight, down_factor, up_factor, own_count, output_gradient
):
    dp_total, fsdp_total = lax.axis_size("dp"), lax.axis_size("fsdp")
    live_rows = jnp.arange(tokens.shape[0], dtype=jnp.int32)[:, None] < own_count
    spare_rows = SLOTS - PAIR_ROWS
    half_bit = dp_total.bit_length() - 2
    kept_rows = jnp.minimum(own_count, PAIR_ROWS)
    guest = partner(take_block(tokens, kept_rows, spare_rows), "dp", half_bit)
    packed = place_block(tokens[:PAIR_ROWS], guest, kept_rows, PAIR_ROWS)
    sliced_rows = lax.all_to_all(packed, "fsdp", split_axis=1, concat_axis=0, tiled=True)
    slice_width = sliced_rows.shape[1]
    all_rows = lax.all_gather(sliced_rows, "dp", axis=0, tiled=True)
    all_rows = all_rows.reshape(dp_total, fsdp_total, PAIR_ROWS, slice_width).swapaxes(0, 1)
    partial_blocks = jnp.dot(
        all_rows.reshape(-1, slice_width), up_weight, preferred_element_type=jnp.float32
    ).astype(jnp.bfloat16)
    blocks = lax.psum_scatter(partial_blocks, "fsdp", scatter_dimension=0, tiled=True)
    paired_base = lax.all_to_all(blocks, "dp", split_axis=0, concat_axis=1, tiled=True)
    returned = partner(take_block(paired_base, kept_rows, spare_rows), "dp", half_bit)
    base_output = place_block(paired_base, returned, kept_rows, SLOTS)
    rank_projection = lax.dot_general(
        tokens, down_factor, (((1,), (1,)), ((), ())), preferred_element_type=jnp.float32
    ).astype(jnp.bfloat16)
    adapter_update = jnp.dot(rank_projection, up_factor, preferred_element_type=jnp.float32)
    hidden_preactivation = base_output.astype(jnp.float32) + LOWRANK_SCALE * adapter_update
    act_out = jnp.where(live_rows, jax.nn.silu(hidden_preactivation), 0.0).astype(jnp.bfloat16)
    grad_pre = jnp.where(
        live_rows, output_gradient.astype(jnp.float32) * silu_slope(hidden_preactivation), 0.0
    ).astype(jnp.bfloat16)
    low_sum = lax.dot_general(
        grad_pre, up_factor, (((1,), (1,)), ((), ())), preferred_element_type=jnp.float32
    )
    second_factor_gradient = LOWRANK_SCALE * lax.dot_general(
        rank_projection, grad_pre, (((0,), (0,)), ((), ())), preferred_element_type=jnp.float32
    )
    return act_out, low_sum, second_factor_gradient


def tail_kernel(
    slots_ref, counts_ref, own_ref, beside_ref, across_ref, diagonal_ref, mix_ref, rank_t_ref,
    factor_ref, cotangent_ref, low_in_ref, *rest
):
    act_ref, second_ref, low_ref, base_ref = rest[-4:]
    which, tile = pl.program_id(0), pl.program_id(1)

    @pl.when((which == 0) & (tile == 0))
    def _():
        low_ref[...] = low_in_ref[...]

    for index, source_ref in enumerate((own_ref, beside_ref, across_ref, diagonal_ref)):

        @pl.when(which == index)
        def _(source_ref=source_ref):
            base_ref[:SLOTS] = source_ref[...]

    factor = factor_ref[...]
    base_ref[SLOTS:] = factor
    inputs = jnp.dot(mix_ref[...], base_ref[...], preferred_element_type=jnp.float32)
    gate_value = jax.nn.sigmoid(inputs)
    live = lax.broadcasted_iota(jnp.int32, inputs.shape, 0) < counts_ref[0]
    kept = jnp.where(live, gate_value, 0.0)
    act = inputs * kept
    act_ref[...] = act.astype(jnp.bfloat16)
    slope = kept + act * (1.0 - gate_value)
    grad_pre = (cotangent_ref[...].astype(jnp.float32) * slope).astype(jnp.bfloat16)
    second_ref[...] = jnp.dot(rank_t_ref[...], grad_pre, preferred_element_type=jnp.float32)
    low_ref[...] += lax.dot_general(
        grad_pre, factor, (((1,), (1,)), ((), ())), preferred_element_type=jnp.float32
    )


def tail(bases, mix, rank_t, factor, cotangent, low, made, slots, count, offset, unit):
    width = bases[0].shape[1]
    rank_total, hidden = factor.shape
    start = offset // unit

    def local(i, t, slots, counts):
        return (0, t)

    def whole(i, t, slots, counts):
        return (0, 0)

    def placed(i, t, slots, counts):
        return (0, slots[i] + start + t)

    in_specs = [pl.BlockSpec((SLOTS, unit), local)] * 4 + [
        pl.BlockSpec(mix.shape, whole),
        pl.BlockSpec(rank_t.shape, whole),
        pl.BlockSpec((rank_total, unit), placed),
        pl.BlockSpec((SLOTS, unit), placed),
        pl.BlockSpec(low.shape, whole),
    ]
    operands = [*bases, mix, rank_t, factor, cotangent, low]
    aliases = {}
    if made is not None:
        in_specs += [pl.BlockSpec(memory_space=pl.ANY)] * 2
        aliases = {2 + len(operands): 0, 3 + len(operands): 1}
        operands += list(made)
    act_out, second, low = pl.pallas_call(
        tail_kernel,
        name="tail",
        out_shape=(
            jax.ShapeDtypeStruct((SLOTS, hidden), jnp.bfloat16),
            jax.ShapeDtypeStruct((rank_total, hidden), jnp.float32),
            jax.ShapeDtypeStruct(low.shape, jnp.float32),
        ),
        grid_spec=pltpu.PrefetchScalarGridSpec(
            num_scalar_prefetch=2,
            grid=(4, width // unit),
            in_specs=in_specs,
            out_specs=(
                pl.BlockSpec((SLOTS, unit), placed),
                pl.BlockSpec((rank_total, unit), placed),
                pl.BlockSpec(low.shape, whole),
            ),
            scratch_shapes=[pltpu.VMEM((SLOTS + rank_total, unit), jnp.bfloat16)],
        ),
        input_output_aliases=aliases,
        cost_estimate=pl.CostEstimate(
            flops=2 * 4 * width * SLOTS * (SLOTS + 3 * rank_total),
            bytes_accessed=4 * width * SLOTS * 8,
            transcendentals=4 * width * SLOTS,
        ),
        compiler_params=pltpu.CompilerParams(
            dimension_semantics=("arbitrary", "arbitrary"), vmem_limit_bytes=6 * 2**20
        ),
    )(slots, count, *operands)
    return (act_out, second), low


CHUNKS = 7
BATCHES = (2, 2, 1, 1, 1)


def prepare_kernel(widths, places_ref, arrange_ref, tokens_ref, *outs):
    index = 0
    for kept_ref, spill_ref in (outs[:2], outs[2:]):
        begin = 0
        for width in widths:
            at = pl.multiple_of(places_ref[index], 128)
            rows = jnp.dot(
                arrange_ref[...], tokens_ref[:, pl.ds(at, width)],
                preferred_element_type=jnp.float32,
            ).astype(jnp.bfloat16)
            kept_ref[:, begin : begin + width] = rows[:PAIR_ROWS]
            spill_ref[:, begin : begin + width] = rows[PAIR_ROWS:]
            begin += width
            index += 1


def prepare(places, widths, arrange, tokens):
    columns = sum(widths)
    kept = jax.ShapeDtypeStruct((PAIR_ROWS, columns), tokens.dtype)
    spill = jax.ShapeDtypeStruct((SLOTS - PAIR_ROWS, columns), tokens.dtype)
    return pl.pallas_call(
        functools.partial(prepare_kernel, widths),
        name="prepare",
        out_shape=(kept, spill, kept, spill),
        grid_spec=pltpu.PrefetchScalarGridSpec(
            num_scalar_prefetch=1,
            grid=(1,),
            in_specs=[
                pl.BlockSpec(arrange.shape, lambda i, places: (0, 0)),
                pl.BlockSpec(tokens.shape, lambda i, places: (0, 0)),
            ],
            out_specs=[
                pl.BlockSpec(out.shape, lambda i, places: (0, 0))
                for out in (kept, spill, kept, spill)
            ],
        ),
        cost_estimate=pl.CostEstimate(
            flops=4 * SLOTS * SLOTS * columns, bytes_accessed=8 * SLOTS * columns, transcendentals=0
        ),
        compiler_params=pltpu.CompilerParams(vmem_limit_bytes=8 * 2**20),
    )(places, arrange, tokens)


def plane_plan(
    tokens, up_weight, down_factor, up_factor, own_count, output_gradient
):
    groups = lax.axis_size("groups")
    place, group = lax.axis_index("fsdp"), lax.axis_index("groups")
    position = lax.axis_index("dp")
    upper = position >= 2
    inner = (place == 1) | (place == 2)
    near = jnp.where(place < 2, 1, 2)
    far = 3 - near
    slice_width, width = up_weight.shape
    part = slice_width // groups
    chunks, batches = CHUNKS, BATCHES
    unit = width // chunks
    spare = SLOTS - PAIR_ROWS
    pair_total = 2 * PAIR_ROWS
    home_total = 2 * pair_total
    beside = [(0, 1), (1, 0), (2, 3), (3, 2)]
    across = [(0, 2), (2, 0), (1, 3), (3, 1)]
    diagonal = [(0, 3), (3, 0), (1, 2), (2, 1)]
    inward = [(0, 1), (3, 2)]
    outward = [(1, 0), (2, 3)]
    middle = [(1, 2), (2, 1)]
    crossing = [(0, 2), (3, 1)]

    row = jnp.arange(SLOTS, dtype=jnp.int32)
    flipped = jnp.where(row < PAIR_ROWS, PAIR_ROWS - 1 - row, SLOTS + PAIR_ROWS - 1 - row)
    arranged = jnp.where(upper, flipped, row)
    arrange = (arranged[:, None] == row[None, :]).astype(jnp.bfloat16)

    def origins(target):
        outer = jnp.where(target < 2, 0, 3)
        return [target * slice_width] + [
            outer * slice_width + lax.rem(group + step, groups) * part for step in range(groups)
        ]

    places = jnp.stack(origins(far) + origins(near)).astype(jnp.int32)
    widths = [slice_width] + [part] * groups
    far_kept, far_spill, near_kept, near_spill = prepare(places, widths, arrange, tokens)
    far_guest = lax.ppermute(far_spill, "dp", across)

    def own_part(weight, c):
        return lax.dynamic_slice(weight, (group * part, c * unit), (part, unit))

    first_weight = after(up_weight, far_spill)
    parts = [own_part(first_weight, c) for c in (0, 1)]
    lines = {0: lax.ppermute(parts[0], "fsdp", inward)}
    near_guest = lax.ppermute(near_spill, "dp", across)

    spot = jnp.where(upper, PAIR_ROWS, 0) + jnp.arange(PAIR_ROWS, dtype=jnp.int32)[:, None]
    is_own = jnp.where(upper, pair_total - 1 - spot, spot) < own_count
    is_guest = (spot >= PAIR_ROWS - spare) & (spot < SLOTS) & ~is_own

    def pack(kept, guest):
        blank = jnp.zeros((PAIR_ROWS - spare, guest.shape[1]), guest.dtype)
        front, back = jnp.concatenate([guest, blank], 0), jnp.concatenate([blank, guest], 0)
        return jnp.where(is_guest, jnp.where(upper, front, back), kept)

    def start_weight(c, *order):
        return lax.ppermute(after(parts[c], *order), "fsdp", inward)

    def share_weight(c, *order):
        line = lines[c]
        pieces = [line]
        line = after(line, *order)
        for step in range(1, groups):
            pairs = [(i, (i - step) % groups) for i in range(groups)]
            pieces.append(lax.ppermute(line, "groups", pairs))
        return pieces

    def ordered_pair(mine):
        theirs = lax.ppermute(mine, "dp", across)
        return jnp.concatenate(
            [jnp.where(upper, theirs, mine), jnp.where(upper, mine, theirs)], 0
        )

    far_columns = pack(far_kept, after(far_guest, parts[0]))
    from_far = lax.ppermute(far_columns, "fsdp", middle)
    near_columns = pack(near_kept, after(near_guest, far_columns))
    near_pair = ordered_pair(near_columns)
    rest_weight = after(up_weight, near_columns)
    parts += [own_part(rest_weight, c) for c in range(2, chunks)]
    rest_weight = after(rest_weight, parts[-1])
    column_weights = [rest_weight[:, :unit]]
    shared = {0: share_weight(0, near_columns)}
    from_far_outer = lax.ppermute(after(far_columns, near_columns), "fsdp", crossing)
    for c in (1, 2):
        lines[c] = start_weight(c, near_columns)
    from_outer = lax.ppermute(near_columns, "fsdp", inward)
    far_pair = ordered_pair(from_far)
    far_rows = jnp.concatenate([far_pair, lax.ppermute(far_pair, "dp", beside)], 0)
    lines[3] = start_weight(3, far_pair)
    outer_pair = ordered_pair(from_far_outer)
    far_outer_rows = jnp.concatenate([outer_pair, lax.ppermute(outer_pair, "dp", beside)], 0)

    def multiply(rows, weight):
        product = jnp.dot(rows, weight, preferred_element_type=jnp.float32)
        return product.astype(jnp.bfloat16)

    weights, sent = {}, {}

    def gather_weight(c):
        weights[c] = jnp.concatenate([column_weights[c]] + shared[c], 0)
        return weights[c]

    rank = lax.dot_general(
        tokens, down_factor, (((1,), (1,)), ((), ())), preferred_element_type=jnp.float32
    ).astype(jnp.bfloat16)
    scaled = (LOWRANK_SCALE * rank).astype(jnp.bfloat16)
    rank_t = scaled.T
    source = jnp.where(upper, SLOTS - 1 - row, row)
    turn = (source[:, None] == row[None, :]).astype(jnp.bfloat16)
    mix = jnp.concatenate([turn, scaled], 1)
    slots = (position ^ jnp.arange(4, dtype=jnp.int32)) * chunks
    low = jnp.zeros((SLOTS, rank.shape[1]), jnp.float32)
    count = own_count.reshape(1)

    first = multiply(far_rows, gather_weight(0))
    first_in = lax.ppermute(first, "fsdp", middle)
    shared[1] = share_weight(1, first)
    rest_weight = after(rest_weight, first)
    column_weights += [rest_weight[:, c * unit : (c + 1) * unit] for c in (1, 2)]
    second = multiply(after(far_outer_rows, first), weights[0])
    second_in = lax.ppermute(second, "fsdp", middle)
    sent[0] = second, jnp.concatenate([first_in, second_in], 0)
    last = second
    rest_weight = after(rest_weight, second)
    column_weights += [rest_weight[:, c * unit : (c + 1) * unit] for c in range(3, chunks)]
    all_far_rows = jnp.concatenate([far_rows, far_outer_rows], 0)
    shared[2] = share_weight(2, last)

    def send_last(c, *order):
        outer = multiply(after(far_outer_rows, *order), gather_weight(c))
        outer_in = lax.ppermute(outer, "fsdp", middle)
        own = multiply(after(far_rows, outer), weights[c])
        sent[c] = outer_in, lax.ppermute(own, "fsdp", middle)
        return own

    def finish_half(c, half, *order):
        rows = after(near_rows[home_total:] if half == 0 else near_rows[:home_total], *order)
        summed = jnp.dot(rows, weights[c], preferred_element_type=jnp.float32)
        return (summed + sent[c][half].astype(jnp.float32)).astype(jnp.bfloat16)

    def send(c, *order):
        outgoing = multiply(after(all_far_rows, *order), gather_weight(c))
        sent[c] = outgoing, lax.ppermute(outgoing, "fsdp", middle)
        return outgoing

    last = send(1, last)
    lines[4] = start_weight(4, last)
    near_outer_pair = ordered_pair(after(from_outer, last))
    last = send(2, last)
    lines[5] = start_weight(5, last)
    shared[3] = share_weight(3, last)
    near_pairs = jnp.concatenate([near_pair, after(near_outer_pair, last)], 0)
    near_others = lax.ppermute(near_pairs, "dp", beside)
    near_rows = jnp.concatenate(
        [near_pair, near_others[:pair_total], near_outer_pair, near_others[pair_total:]], 0
    )

    def finish(c, *order):
        rows = after(near_rows, *order)
        summed = jnp.dot(rows, weights[c], preferred_element_type=jnp.float32)
        summed = (summed + sent[c][1].astype(jnp.float32)).astype(jnp.bfloat16)
        return summed, lax.ppermute(summed[home_total:], "fsdp", outward)

    def hand_out(members, *order):
        handed = [after(handed, *order) for _, handed in members]
        homes = [
            jnp.where(inner, summed[:home_total], back)
            for (summed, _), back in zip(members, handed, strict=True)
        ]
        home = jnp.concatenate(homes, 1).reshape(2, pair_total, -1)
        shape = (1, SLOTS, home.shape[2])
        low_at, high_at = jnp.int32(0), jnp.int32(pair_total - SLOTS)
        same, other = jnp.where(upper, high_at, low_at), jnp.where(upper, low_at, high_at)
        cuts = [
            lax.dynamic_slice(home, (pair, row_at, 0), shape)[0]
            for pair, row_at in ((0, same), (1, same), (0, other), (1, other))
        ]
        opposite = lax.ppermute(cuts[2], "dp", across)
        cornered = lax.ppermute(cuts[3], "dp", diagonal)
        adjacent = lax.ppermute(cuts[1], "dp", beside)
        return cuts, [cuts[0], adjacent, opposite, cornered]

    batch_ends = [sum(batches[: b + 1]) - 1 for b in range(len(batches))]
    made = None
    summed, pending = {}, []

    def finish_tail(last):
        nonlocal made, low
        bases, offset = pending.pop(0)
        bases[3] = after(bases[3], last)
        made, low = tail(
            bases, mix, rank_t, up_factor, output_gradient, low, made, slots, count,
            offset, unit,
        )
        return low

    def hand_batch(c, last):
        if c not in batch_ends:
            return last
        b = batch_ends.index(c)
        begin = batch_ends[b] - batches[b] + 1
        cuts, bases = hand_out([summed[c] for c in range(begin, c + 1)], last)
        pending.append((bases, begin * unit))
        return cuts[0]

    final = chunks - 1
    for i in range(final):
        summed[i] = finish(i, last)
        last = summed[i][0]
        if i + 6 < chunks:
            lines[i + 6] = start_weight(i + 6, last)
        if i + 4 < chunks:
            shared[i + 4] = share_weight(i + 4, last)
        if i + 3 < final:
            last = send(i + 3, last)
        elif i + 3 == final:
            last = send_last(final, last)
        if i > 0:
            last = hand_batch(i - 1, last)
    outer_sum = finish_half(final, 0, last)
    handed = lax.ppermute(outer_sum, "fsdp", outward)
    last = finish_tail(outer_sum)
    last = hand_batch(final - 1, last)
    own_sum = finish_half(final, 1, last)
    summed[final] = own_sum, handed
    last = hand_batch(final, own_sum)
    while pending:
        last = finish_tail(last)
    return made[0], low, made[1]


def per_device(
    plane, tokens, up_weight, first_adapter_factors, second_adapter_factors, counts, output_gradient
):
    slice_width, width = up_weight.shape
    fits = width % (CHUNKS * 128) == 0 and slice_width % (128 * lax.axis_size("groups")) == 0
    plan = plane_plan if plane and fits else scattered_plan
    act_out, low_sum, second_factor_gradient = plan(
        tokens, up_weight, first_adapter_factors[0], second_adapter_factors[0], counts[0],
        output_gradient,
    )
    low_rank_gradient = (LOWRANK_SCALE * low_sum).astype(jnp.bfloat16)
    grad_a = lax.dot_general(
        low_rank_gradient, tokens, (((0,), (0,)), ((), ())), preferred_element_type=jnp.float32
    )
    return (act_out, grad_a[None], second_factor_gradient[None])


def solution(mesh):
    placed = (
        P(("groups", "dp", "fsdp"), None),
        P("fsdp", "dp"),
        P(("groups", "dp", "fsdp"), None, None),
        P(("groups", "dp", "fsdp"), None, None),
        P(("groups", "dp", "fsdp")),
        P(("groups", "dp", "fsdp"), None),
    )

    plane = mesh.shape["fsdp"] == 4 and mesh.shape["dp"] == 4
    return jax.shard_map(
        functools.partial(per_device, plane),
        mesh=mesh,
        in_specs=placed,
        out_specs=(
            P(("groups", "dp", "fsdp"), None),
            P(("groups", "dp", "fsdp"), None, None),
            P(("groups", "dp", "fsdp"), None, None),
        ),
        check_vma=False,
    )
```

```python
import functools

import jax
import jax.numpy as jnp
from jax import lax
from jax.experimental import pallas as pl
from jax.experimental.pallas import tpu as pltpu
from jax.sharding import PartitionSpec as P


SLOTS = 128
PAIR_ROWS = 80


LOWRANK_SCALE = 2.0


def partner(x, axis, distance):
    return lax.ppermute(x, axis, [(i, i ^ 1 << distance) for i in range(lax.axis_size(axis))])


def silu_slope(inputs):
    gate_value = jax.nn.sigmoid(inputs)
    return gate_value * (1.0 + inputs * (1.0 - gate_value))


def take_block(rows_all, offset, row_count):
    filler = jnp.zeros((row_count,) + rows_all.shape[1:], rows_all.dtype)
    padded = jnp.concatenate([rows_all, filler], 0)
    return lax.dynamic_slice_in_dim(padded, offset, row_count, 0)


def place_block(rows_kept, block, offset, row_total):
    filler = jnp.zeros((block.shape[0],) + rows_kept.shape[1:], rows_kept.dtype)
    padded = jnp.concatenate([rows_kept, filler], 0)
    placed = lax.dynamic_update_slice_in_dim(padded, block, offset, 0)
    return placed[:row_total]


def after(x, *others):
    return lax.optimization_barrier((x,) + others)[0]


def scattered_plan(
    tokens, up_weight, down_factor, up_factor, own_count, output_gradient
):
    dp_total, fsdp_total = lax.axis_size("dp"), lax.axis_size("fsdp")
    live_rows = jnp.arange(tokens.shape[0], dtype=jnp.int32)[:, None] < own_count
    spare_rows = SLOTS - PAIR_ROWS
    half_bit = dp_total.bit_length() - 2
    kept_rows = jnp.minimum(own_count, PAIR_ROWS)
    guest = partner(take_block(tokens, kept_rows, spare_rows), "dp", half_bit)
    packed = place_block(tokens[:PAIR_ROWS], guest, kept_rows, PAIR_ROWS)
    sliced_rows = lax.all_to_all(packed, "fsdp", split_axis=1, concat_axis=0, tiled=True)
    slice_width = sliced_rows.shape[1]
    all_rows = lax.all_gather(sliced_rows, "dp", axis=0, tiled=True)
    all_rows = all_rows.reshape(dp_total, fsdp_total, PAIR_ROWS, slice_width).swapaxes(0, 1)
    partial_blocks = jnp.dot(
        all_rows.reshape(-1, slice_width), up_weight, preferred_element_type=jnp.float32
    ).astype(jnp.bfloat16)
    blocks = lax.psum_scatter(partial_blocks, "fsdp", scatter_dimension=0, tiled=True)
    paired_base = lax.all_to_all(blocks, "dp", split_axis=0, concat_axis=1, tiled=True)
    returned = partner(take_block(paired_base, kept_rows, spare_rows), "dp", half_bit)
    base_output = place_block(paired_base, returned, kept_rows, SLOTS)
    rank_projection = lax.dot_general(
        tokens, down_factor, (((1,), (1,)), ((), ())), preferred_element_type=jnp.float32
    ).astype(jnp.bfloat16)
    adapter_update = jnp.dot(rank_projection, up_factor, preferred_element_type=jnp.float32)
    hidden_preactivation = base_output.astype(jnp.float32) + LOWRANK_SCALE * adapter_update
    act_out = jnp.where(live_rows, jax.nn.silu(hidden_preactivation), 0.0).astype(jnp.bfloat16)
    grad_pre = jnp.where(
        live_rows, output_gradient.astype(jnp.float32) * silu_slope(hidden_preactivation), 0.0
    ).astype(jnp.bfloat16)
    low_sum = lax.dot_general(
        grad_pre, up_factor, (((1,), (1,)), ((), ())), preferred_element_type=jnp.float32
    )
    second_factor_gradient = LOWRANK_SCALE * lax.dot_general(
        rank_projection, grad_pre, (((0,), (0,)), ((), ())), preferred_element_type=jnp.float32
    )
    return act_out, low_sum, second_factor_gradient


def tail_kernel(
    slots_ref, counts_ref, own_ref, beside_ref, across_ref, diagonal_ref, mix_ref, rank_t_ref,
    factor_ref, cotangent_ref, low_in_ref, *rest
):
    act_ref, second_ref, low_ref, base_ref = rest[-4:]
    which, tile = pl.program_id(0), pl.program_id(1)

    @pl.when((which == 0) & (tile == 0))
    def _():
        low_ref[...] = low_in_ref[...]

    for index, source_ref in enumerate((own_ref, beside_ref, across_ref, diagonal_ref)):

        @pl.when(which == index)
        def _(source_ref=source_ref):
            base_ref[:SLOTS] = source_ref[...]

    factor = factor_ref[...]
    base_ref[SLOTS:] = factor
    inputs = jnp.dot(mix_ref[...], base_ref[...], preferred_element_type=jnp.float32)
    gate_value = jax.nn.sigmoid(inputs)
    live = lax.broadcasted_iota(jnp.int32, inputs.shape, 0) < counts_ref[0]
    kept = jnp.where(live, gate_value, 0.0)
    act = inputs * kept
    act_ref[...] = act.astype(jnp.bfloat16)
    slope = kept + act * (1.0 - gate_value)
    grad_pre = (cotangent_ref[...].astype(jnp.float32) * slope).astype(jnp.bfloat16)
    second_ref[...] = jnp.dot(rank_t_ref[...], grad_pre, preferred_element_type=jnp.float32)
    low_ref[...] += lax.dot_general(
        grad_pre, factor, (((1,), (1,)), ((), ())), preferred_element_type=jnp.float32
    )


def tail(bases, mix, rank_t, factor, cotangent, low, made, slots, count, offset, unit):
    width = bases[0].shape[1]
    rank_total, hidden = factor.shape
    start = offset // unit

    def local(i, t, slots, counts):
        return (0, t)

    def whole(i, t, slots, counts):
        return (0, 0)

    def placed(i, t, slots, counts):
        return (0, slots[i] + start + t)

    in_specs = [pl.BlockSpec((SLOTS, unit), local)] * 4 + [
        pl.BlockSpec(mix.shape, whole),
        pl.BlockSpec(rank_t.shape, whole),
        pl.BlockSpec((rank_total, unit), placed),
        pl.BlockSpec((SLOTS, unit), placed),
        pl.BlockSpec(low.shape, whole),
    ]
    operands = [*bases, mix, rank_t, factor, cotangent, low]
    aliases = {}
    if made is not None:
        in_specs += [pl.BlockSpec(memory_space=pl.ANY)] * 2
        aliases = {2 + len(operands): 0, 3 + len(operands): 1}
        operands += list(made)
    act_out, second, low = pl.pallas_call(
        tail_kernel,
        name="tail",
        out_shape=(
            jax.ShapeDtypeStruct((SLOTS, hidden), jnp.bfloat16),
            jax.ShapeDtypeStruct((rank_total, hidden), jnp.float32),
            jax.ShapeDtypeStruct(low.shape, jnp.float32),
        ),
        grid_spec=pltpu.PrefetchScalarGridSpec(
            num_scalar_prefetch=2,
            grid=(4, width // unit),
            in_specs=in_specs,
            out_specs=(
                pl.BlockSpec((SLOTS, unit), placed),
                pl.BlockSpec((rank_total, unit), placed),
                pl.BlockSpec(low.shape, whole),
            ),
            scratch_shapes=[pltpu.VMEM((SLOTS + rank_total, unit), jnp.bfloat16)],
        ),
        input_output_aliases=aliases,
        cost_estimate=pl.CostEstimate(
            flops=2 * 4 * width * SLOTS * (SLOTS + 3 * rank_total),
            bytes_accessed=4 * width * SLOTS * 8,
            transcendentals=4 * width * SLOTS,
        ),
        compiler_params=pltpu.CompilerParams(
            dimension_semantics=("arbitrary", "arbitrary"), vmem_limit_bytes=6 * 2**20
        ),
    )(slots, count, *operands)
    return (act_out, second), low


CHUNKS = 7
BATCHES = (2, 2, 1, 1, 1)


def prepare_kernel(widths, places_ref, arrange_ref, tokens_ref, *outs):
    index = 0
    for kept_ref, spill_ref in (outs[:2], outs[2:]):
        begin = 0
        for width in widths:
            at = pl.multiple_of(places_ref[index], 128)
            rows = jnp.dot(
                arrange_ref[...], tokens_ref[:, pl.ds(at, width)],
                preferred_element_type=jnp.float32,
            ).astype(jnp.bfloat16)
            kept_ref[:, begin : begin + width] = rows[:PAIR_ROWS]
            spill_ref[:, begin : begin + width] = rows[PAIR_ROWS:]
            begin += width
            index += 1


def prepare(places, widths, arrange, tokens):
    columns = sum(widths)
    kept = jax.ShapeDtypeStruct((PAIR_ROWS, columns), tokens.dtype)
    spill = jax.ShapeDtypeStruct((SLOTS - PAIR_ROWS, columns), tokens.dtype)
    return pl.pallas_call(
        functools.partial(prepare_kernel, widths),
        name="prepare",
        out_shape=(kept, spill, kept, spill),
        grid_spec=pltpu.PrefetchScalarGridSpec(
            num_scalar_prefetch=1,
            grid=(1,),
            in_specs=[
                pl.BlockSpec(arrange.shape, lambda i, places: (0, 0)),
                pl.BlockSpec(tokens.shape, lambda i, places: (0, 0)),
            ],
            out_specs=[
                pl.BlockSpec(out.shape, lambda i, places: (0, 0))
                for out in (kept, spill, kept, spill)
            ],
        ),
        cost_estimate=pl.CostEstimate(
            flops=4 * SLOTS * SLOTS * columns, bytes_accessed=8 * SLOTS * columns, transcendentals=0
        ),
        compiler_params=pltpu.CompilerParams(vmem_limit_bytes=8 * 2**20),
    )(places, arrange, tokens)


def plane_plan(
    tokens, up_weight, down_factor, up_factor, own_count, output_gradient
):
    groups = lax.axis_size("groups")
    place, group = lax.axis_index("fsdp"), lax.axis_index("groups")
    position = lax.axis_index("dp")
    upper = position >= 2
    inner = (place == 1) | (place == 2)
    near = jnp.where(place < 2, 1, 2)
    far = 3 - near
    slice_width, width = up_weight.shape
    part = slice_width // groups
    chunks, batches = CHUNKS, BATCHES
    unit = width // chunks
    spare = SLOTS - PAIR_ROWS
    pair_total = 2 * PAIR_ROWS
    home_total = 2 * pair_total
    beside = [(0, 1), (1, 0), (2, 3), (3, 2)]
    across = [(0, 2), (2, 0), (1, 3), (3, 1)]
    diagonal = [(0, 3), (3, 0), (1, 2), (2, 1)]
    inward = [(0, 1), (3, 2)]
    outward = [(1, 0), (2, 3)]
    middle = [(1, 2), (2, 1)]
    crossing = [(0, 2), (3, 1)]

    row = jnp.arange(SLOTS, dtype=jnp.int32)
    flipped = jnp.where(row < PAIR_ROWS, PAIR_ROWS - 1 - row, SLOTS + PAIR_ROWS - 1 - row)
    arranged = jnp.where(upper, flipped, row)
    arrange = (arranged[:, None] == row[None, :]).astype(jnp.bfloat16)

    def origins(target):
        outer = jnp.where(target < 2, 0, 3)
        return [target * slice_width] + [
            outer * slice_width + lax.rem(group + step, groups) * part for step in range(groups)
        ]

    places = jnp.stack(origins(far) + origins(near)).astype(jnp.int32)
    widths = [slice_width] + [part] * groups
    far_kept, far_spill, near_kept, near_spill = prepare(places, widths, arrange, tokens)
    far_guest = lax.ppermute(far_spill, "dp", across)

    def own_part(weight, c):
        return lax.dynamic_slice(weight, (group * part, c * unit), (part, unit))

    first_weight = after(up_weight, far_spill)
    parts = [own_part(first_weight, c) for c in (0, 1)]
    lines = {0: lax.ppermute(parts[0], "fsdp", inward)}
    near_guest = lax.ppermute(near_spill, "dp", across)

    spot = jnp.where(upper, PAIR_ROWS, 0) + jnp.arange(PAIR_ROWS, dtype=jnp.int32)[:, None]
    is_own = jnp.where(upper, pair_total - 1 - spot, spot) < own_count
    is_guest = (spot >= PAIR_ROWS - spare) & (spot < SLOTS) & ~is_own

    def pack(kept, guest):
        blank = jnp.zeros((PAIR_ROWS - spare, guest.shape[1]), guest.dtype)
        front, back = jnp.concatenate([guest, blank], 0), jnp.concatenate([blank, guest], 0)
        return jnp.where(is_guest, jnp.where(upper, front, back), kept)

    def start_weight(c, *order):
        return lax.ppermute(after(parts[c], *order), "fsdp", inward)

    def share_weight(c, *order):
        line = lines[c]
        pieces = [line]
        line = after(line, *order)
        for step in range(1, groups):
            pairs = [(i, (i - step) % groups) for i in range(groups)]
            pieces.append(lax.ppermute(line, "groups", pairs))
        return pieces

    def ordered_pair(mine):
        theirs = lax.ppermute(mine, "dp", across)
        return jnp.concatenate(
            [jnp.where(upper, theirs, mine), jnp.where(upper, mine, theirs)], 0
        )

    far_columns = pack(far_kept, after(far_guest, parts[0]))
    from_far = lax.ppermute(far_columns, "fsdp", middle)
    near_columns = pack(near_kept, after(near_guest, far_columns))
    near_pair = ordered_pair(near_columns)
    rest_weight = after(up_weight, near_columns)
    parts += [own_part(rest_weight, c) for c in range(2, chunks)]
    rest_weight = after(rest_weight, parts[-1])
    column_weights = [rest_weight[:, :unit]]
    shared = {0: share_weight(0, near_columns)}
    from_far_outer = lax.ppermute(after(far_columns, near_columns), "fsdp", crossing)
    for c in (1, 2):
        lines[c] = start_weight(c, near_columns)
    from_outer = lax.ppermute(near_columns, "fsdp", inward)
    far_pair = ordered_pair(from_far)
    far_rows = jnp.concatenate([far_pair, lax.ppermute(far_pair, "dp", beside)], 0)
    lines[3] = start_weight(3, far_pair)
    near_others = lax.ppermute(near_pair, "dp", beside)
    outer_pair = ordered_pair(from_far_outer)
    far_outer_rows = jnp.concatenate([outer_pair, lax.ppermute(outer_pair, "dp", beside)], 0)

    def multiply(rows, weight):
        product = jnp.dot(rows, weight, preferred_element_type=jnp.float32)
        return product.astype(jnp.bfloat16)

    weights, sent = {}, {}

    def gather_weight(c):
        weights[c] = jnp.concatenate([column_weights[c]] + shared[c], 0)
        return weights[c]

    rank = lax.dot_general(
        tokens, down_factor, (((1,), (1,)), ((), ())), preferred_element_type=jnp.float32
    ).astype(jnp.bfloat16)
    scaled = (LOWRANK_SCALE * rank).astype(jnp.bfloat16)
    rank_t = scaled.T
    source = jnp.where(upper, SLOTS - 1 - row, row)
    turn = (source[:, None] == row[None, :]).astype(jnp.bfloat16)
    mix = jnp.concatenate([turn, scaled], 1)
    slots = (position ^ jnp.arange(4, dtype=jnp.int32)) * chunks
    low = jnp.zeros((SLOTS, rank.shape[1]), jnp.float32)
    count = own_count.reshape(1)

    first = multiply(far_rows, gather_weight(0))
    first_in = lax.ppermute(first, "fsdp", middle)
    shared[1] = share_weight(1, first)
    rest_weight = after(rest_weight, first)
    column_weights += [rest_weight[:, c * unit : (c + 1) * unit] for c in (1, 2)]
    second = multiply(after(far_outer_rows, first), weights[0])
    second_in = lax.ppermute(second, "fsdp", middle)
    sent[0] = second, jnp.concatenate([first_in, second_in], 0)
    last = second
    rest_weight = after(rest_weight, second)
    column_weights += [rest_weight[:, c * unit : (c + 1) * unit] for c in range(3, chunks)]
    all_far_rows = jnp.concatenate([far_rows, far_outer_rows], 0)
    shared[2] = share_weight(2, last)

    def send_last(c, *order):
        outer = multiply(after(far_outer_rows, *order), gather_weight(c))
        outer_in = lax.ppermute(outer, "fsdp", middle)
        own = multiply(after(far_rows, outer), weights[c])
        sent[c] = outer_in, lax.ppermute(own, "fsdp", middle)
        return own

    def finish_half(c, half, *order):
        rows = after(near_rows[home_total:] if half == 0 else near_rows[:home_total], *order)
        summed = jnp.dot(rows, weights[c], preferred_element_type=jnp.float32)
        return (summed + sent[c][half].astype(jnp.float32)).astype(jnp.bfloat16)

    def send(c, *order):
        outgoing = multiply(after(all_far_rows, *order), gather_weight(c))
        sent[c] = outgoing, lax.ppermute(outgoing, "fsdp", middle)
        return outgoing

    last = send(1, last)
    lines[4] = start_weight(4, last)
    outer_pair = ordered_pair(after(from_outer, last))
    last = send(2, last)
    lines[5] = start_weight(5, last)
    shared[3] = share_weight(3, last)
    outer_pair = after(outer_pair, last)
    near_rows = jnp.concatenate(
        [near_pair, near_others, outer_pair, lax.ppermute(outer_pair, "dp", beside)], 0
    )
    last = send(3, last)
    lines[6] = start_weight(6, last)
    shared[4] = share_weight(4, last)

    def finish(c, *order):
        rows = after(near_rows, *order)
        summed = jnp.dot(rows, weights[c], preferred_element_type=jnp.float32)
        summed = (summed + sent[c][1].astype(jnp.float32)).astype(jnp.bfloat16)
        return summed, lax.ppermute(summed[home_total:], "fsdp", outward)

    def hand_out(members, *order):
        handed = [after(handed, *order) for _, handed in members]
        homes = [
            jnp.where(inner, summed[:home_total], back)
            for (summed, _), back in zip(members, handed, strict=True)
        ]
        home = jnp.concatenate(homes, 1).reshape(2, pair_total, -1)
        shape = (1, SLOTS, home.shape[2])
        low_at, high_at = jnp.int32(0), jnp.int32(pair_total - SLOTS)
        same, other = jnp.where(upper, high_at, low_at), jnp.where(upper, low_at, high_at)
        cuts = [
            lax.dynamic_slice(home, (pair, row_at, 0), shape)[0]
            for pair, row_at in ((0, same), (1, same), (0, other), (1, other))
        ]
        opposite = lax.ppermute(cuts[2], "dp", across)
        cornered = lax.ppermute(cuts[3], "dp", diagonal)
        adjacent = lax.ppermute(cuts[1], "dp", beside)
        return cuts, [cuts[0], adjacent, opposite, cornered]

    batch_ends = [sum(batches[: b + 1]) - 1 for b in range(len(batches))]
    made = None
    summed, pending = {}, []

    def finish_tail(last):
        nonlocal made, low
        bases, offset = pending.pop(0)
        bases[3] = after(bases[3], last)
        made, low = tail(
            bases, mix, rank_t, up_factor, output_gradient, low, made, slots, count,
            offset, unit,
        )
        return low

    def hand_batch(c, last):
        if c not in batch_ends:
            return last
        b = batch_ends.index(c)
        begin = batch_ends[b] - batches[b] + 1
        cuts, bases = hand_out([summed[c] for c in range(begin, c + 1)], last)
        pending.append((bases, begin * unit))
        return cuts[0]

    final = chunks - 1

    def finish_next(i, last):
        summed[i] = finish(i, last)
        return summed[i][0]

    last = finish_next(0, last)
    last = finish_next(1, last)
    shared[5] = share_weight(5, last)
    last = send(4, last)
    last = finish_next(2, last)
    shared[6] = share_weight(6, last)
    last = send(5, last)
    last = finish_next(3, last)
    last = hand_batch(1, last)
    last = finish_next(4, last)
    last = send_last(final, last)
    last = hand_batch(3, last)
    last = finish_next(5, last)
    outer_sum = finish_half(final, 0, last)
    handed = lax.ppermute(outer_sum, "fsdp", outward)
    last = hand_batch(4, outer_sum)
    last = finish_tail(last)
    own_sum = finish_half(final, 1, last)
    summed[final] = own_sum, handed
    last = hand_batch(final - 1, own_sum)
    last = hand_batch(final, last)
    while pending:
        last = finish_tail(last)
    return made[0], low, made[1]


def per_device(
    plane, tokens, up_weight, first_adapter_factors, second_adapter_factors, counts, output_gradient
):
    slice_width, width = up_weight.shape
    fits = width % (CHUNKS * 128) == 0 and slice_width % (128 * lax.axis_size("groups")) == 0
    plan = plane_plan if plane and fits else scattered_plan
    act_out, low_sum, second_factor_gradient = plan(
        tokens, up_weight, first_adapter_factors[0], second_adapter_factors[0], counts[0],
        output_gradient,
    )
    low_rank_gradient = (LOWRANK_SCALE * low_sum).astype(jnp.bfloat16)
    grad_a = lax.dot_general(
        low_rank_gradient, tokens, (((0,), (0,)), ((), ())), preferred_element_type=jnp.float32
    )
    return (act_out, grad_a[None], second_factor_gradient[None])


def solution(mesh):
    placed = (
        P(("groups", "dp", "fsdp"), None),
        P("fsdp", "dp"),
        P(("groups", "dp", "fsdp"), None, None),
        P(("groups", "dp", "fsdp"), None, None),
        P(("groups", "dp", "fsdp")),
        P(("groups", "dp", "fsdp"), None),
    )

    plane = mesh.shape["fsdp"] == 4 and mesh.shape["dp"] == 4
    return jax.shard_map(
        functools.partial(per_device, plane),
        mesh=mesh,
        in_specs=placed,
        out_specs=(
            P(("groups", "dp", "fsdp"), None),
            P(("groups", "dp", "fsdp"), None, None),
            P(("groups", "dp", "fsdp"), None, None),
        ),
        check_vma=False,
    )
```
